16 devices in a mesh: dp: 2 (over y, z), tp: 8 (over x, core).
Axes of the slice: x: 4, y: 2, z: 1, core: 2. Of those that a mesh axis runs over, the one named last changes fastest.
The devices are a block of a 4x4x8 slice.
Arguments:
- x_in: bfloat16 [2, 2048, 1024], P(None, ('dp', 'tp')), parts along dimension 1
- y_cot: bfloat16 [2, 2048, 1024], P(None, ('dp', 'tp')), parts along dimension 1
- gain_attn: float32 [2, 1024], replicated
- gain_mlp: float32 [2, 1024], replicated
- w_qkv: bfloat16 [2, 1024, 8, 4, 128], P(None, None, 'tp')
- w_out: bfloat16 [2, 16, 128, 1024], P(None, 'tp')
- w_gate: bfloat16 [2, 1024, 3072], P(None, None, 'tp')
- w_up: bfloat16 [2, 1024, 3072], P(None, None, 'tp')
- w_down: bfloat16 [2, 3072, 1024], P(None, 'tp')
Outputs:
- output 1: bfloat16 [2, 2048, 1024], P(None, ('dp', 'tp')), parts along dimension 1
- output 2: bfloat16 [2, 2048, 1024], P(None, ('dp', 'tp')), parts along dimension 1
- output 3: bfloat16 [4, 1024, 8, 4, 128], P('dp', None, 'tp'), parts along dimension 0
- output 4: bfloat16 [4, 16, 128, 1024], P('dp', 'tp'), parts along dimension 0
- output 5: bfloat16 [4, 1024, 3072], P('dp', None, 'tp'), parts along dimension 0
- output 6: bfloat16 [4, 1024, 3072], P('dp', None, 'tp'), parts along dimension 0
- output 7: bfloat16 [4, 3072, 1024], P('dp', 'tp'), parts along dimension 0
- output 8: float32 [4, 1024], P('dp'), parts along dimension 0
- output 9: float32 [4, 1024], P('dp'), parts along dimension 0
There are 2 independent parts. The reference program is written for one: setup_inputs(seed, part) draws one part's arguments, and reference() takes and returns one part's arrays. A program takes and returns all parts, laid end to end along the dimension named above; an argument that names none is the same for every part.
All inputs are finite; a program needn't handle non-finite values.
Results may differ from the reference program's by a relative error of at most 0.02.
Values are sent between devices in bfloat16 or wider.
A program may use at most 768 MiB of HBM per device.

```python
import jax
import jax.numpy as jnp
from jax import lax

D = 1024
FF = 3072
HEADS = 16
KV_HEADS = 8
HEAD = 128
SEQ = 1024
LAYERS = 2
MICRO = 2
GROUP = HEADS // KV_HEADS
NORM_EPS = 1e-5


def setup_inputs(seed: int = 0, part: int = 0) -> dict:
    base_key = jax.random.key(seed)
    shared_keys = jax.random.split(base_key, 7)
    part_keys = jax.random.split(jax.random.fold_in(base_key, part), 2)
    x_in = jax.random.normal(part_keys[0], (MICRO, SEQ, D), jnp.float32)
    y_cot = jax.random.normal(part_keys[1], (MICRO, SEQ, D), jnp.float32)
    gain_attn = 1.0 + 0.3 * jax.random.normal(shared_keys[0], (LAYERS, D), jnp.float32)
    gain_mlp = 1.0 + 0.3 * jax.random.normal(shared_keys[1], (LAYERS, D), jnp.float32)
    w_qkv = jax.random.normal(shared_keys[2], (LAYERS, D, KV_HEADS, GROUP + 2, HEAD), jnp.float32) * D ** -0.5
    w_out = jax.random.normal(shared_keys[3], (LAYERS, HEADS, HEAD, D), jnp.float32) * (HEADS * HEAD) ** -0.5
    w_gate = jax.random.normal(shared_keys[4], (LAYERS, D, FF), jnp.float32) * D ** -0.5
    w_up = jax.random.normal(shared_keys[5], (LAYERS, D, FF), jnp.float32) * D ** -0.5
    w_down = jax.random.normal(shared_keys[6], (LAYERS, FF, D), jnp.float32) * FF ** -0.5
    return {'x_in': x_in.astype(jnp.bfloat16), 'y_cot': y_cot.astype(jnp.bfloat16), 'gain_attn': gain_attn, 'gain_mlp': gain_mlp, 'w_qkv': w_qkv.astype(jnp.bfloat16), 'w_out': w_out.astype(jnp.bfloat16), 'w_gate': w_gate.astype(jnp.bfloat16), 'w_up': w_up.astype(jnp.bfloat16), 'w_down': w_down.astype(jnp.bfloat16)}


def rms_norm(row_vals, gain_vec):
    return row_vals * lax.rsqrt(jnp.mean(row_vals * row_vals, axis=-1, keepdims=True) + NORM_EPS) * gain_vec


def group_attention(queries, key_rows, value_rows):
    scores = jnp.einsum('qge,ke->gqk', queries.astype(jnp.float32), key_rows.astype(jnp.float32)) * HEAD ** -0.5
    positions = jnp.arange(SEQ)
    scores = jnp.where(positions[:, None] >= positions[None, :], scores, -1e30)
    prob_b16 = jax.nn.softmax(scores, axis=-1).astype(jnp.bfloat16)
    attn_mix = jnp.einsum('gqk,ke->qge', prob_b16.astype(jnp.float32), value_rows.astype(jnp.float32))
    return attn_mix.astype(jnp.bfloat16)


attention_ckpt = jax.checkpoint(group_attention)


def group_step(group_args):
    return attention_ckpt(group_args[0], group_args[1], group_args[2])


def layer_forward(layer_in, layer_params):
    gain_first, gain_second, qkv_weight, out_weight, gate_weight, up_weight, down_weight = layer_params
    x_f32 = layer_in.astype(jnp.float32)
    normed = rms_norm(x_f32, gain_first).astype(jnp.bfloat16)
    qkv_heads = jnp.einsum('sd,dkje->skje', normed.astype(jnp.float32), qkv_weight).astype(jnp.bfloat16)
    attn_mix = lax.map(group_step, (jnp.swapaxes(qkv_heads[:, :, :GROUP], 0, 1), jnp.swapaxes(qkv_heads[:, :, GROUP], 0, 1), jnp.swapaxes(qkv_heads[:, :, GROUP + 1], 0, 1)))
    attn_sum = jnp.einsum('kqge,kged->qd', attn_mix.astype(jnp.float32), out_weight.reshape(KV_HEADS, GROUP, HEAD, D))
    hidden = (x_f32 + attn_sum.astype(jnp.bfloat16).astype(jnp.float32)).astype(jnp.bfloat16)
    normed_b = rms_norm(hidden.astype(jnp.float32), gain_second).astype(jnp.bfloat16)
    gate_pre = jnp.dot(normed_b.astype(jnp.float32), gate_weight, preferred_element_type=jnp.float32)
    up_proj = jnp.dot(normed_b.astype(jnp.float32), up_weight, preferred_element_type=jnp.float32)
    inner = (jax.nn.silu(gate_pre) * up_proj).astype(jnp.bfloat16)
    down_sum = jnp.dot(inner.astype(jnp.float32), down_weight, preferred_element_type=jnp.float32).astype(jnp.bfloat16)
    return (hidden.astype(jnp.float32) + down_sum.astype(jnp.float32)).astype(jnp.bfloat16)


def stack_forward(layer_in, params):
    def layer_body(carry, layer_params):
        return layer_forward(carry, layer_params), None
    final_rows, unused = lax.scan(layer_body, layer_in, params)
    return final_rows


def reference(x_in, y_cot, gain_attn, gain_mlp, w_qkv, w_out, w_gate, w_up, w_down):
    params = (gain_attn, gain_mlp, w_qkv.astype(jnp.float32), w_out.astype(jnp.float32), w_gate.astype(jnp.float32), w_up.astype(jnp.float32), w_down.astype(jnp.float32))
    first_out, first_pull = jax.vjp(stack_forward, x_in[0], params)
    first_rows, first_grads = first_pull(y_cot[0])
    second_out, second_pull = jax.vjp(stack_forward, x_in[1], params)
    second_rows, second_grads = second_pull(y_cot[1])
    summed = [grad_one + grad_two for grad_one, grad_two in zip(first_grads, second_grads)]
    return (jnp.stack([first_out, second_out]), jnp.stack([first_rows, second_rows]), summed[2].astype(jnp.bfloat16), summed[3].astype(jnp.bfloat16), summed[4].astype(jnp.bfloat16), summed[5].astype(jnp.bfloat16), summed[6].astype(jnp.bfloat16), summed[0], summed[1])
```

```python
import functools

import jax
import jax.numpy as jnp
from jax import lax
from jax.experimental import pallas as pl
from jax.experimental.pallas import tpu as pltpu
from jax.sharding import PartitionSpec as P

NORM_EPS = 1e-5
MESH = pl.DeviceIdType.MESH
BF16 = jnp.bfloat16
F32 = jnp.float32
VMEM_BYTES = 67043328
HEAD = 128
SPLITS = ()

(XR, UR, HR, VR, YR, GR, FN, FS, PREC, RFU, RFD, RU, RD, SA, SB, QKV, MIX, LSE, GP,
 WQ, WO, W1, W3, W2, GA, GM, AQ, AO, A1, A3, A2, BQ, BO, B1, B3, B2, PART, DQKV, DK, DV, GBUF, GSUM) = range(42)


def dot_nn(a, b):
    return lax.dot_general(a, b, (((1,), (0,)), ((), ())), preferred_element_type=F32)


def dot_nt(a, b):
    return lax.dot_general(a, b, (((1,), (1,)), ((), ())), preferred_element_type=F32)


def dot_tn(a, b):
    return lax.dot_general(a, b, (((0,), (0,)), ((), ())), preferred_element_type=F32)


def norm_rows(rows, gain):
    return rows * lax.rsqrt(jnp.mean(rows * rows, axis=-1, keepdims=True) + NORM_EPS) * gain


class Plan:
    def __init__(self, count, micro, layers, rows, width, qkv_w, mix_w, ff):
        self.count, self.micro, self.layers, self.rows, self.width = count, micro, layers, rows, width
        self.qkv_w, self.mix_w, self.ff = qkv_w, mix_w, ff
        self.chips = count // 2
        self.steps = 4 * layers
        self.seq = [(m, k) for k in range(self.steps + 1) for m in range(micro)]

    def shape(self, key):
        kind = key[0]
        c, r, w = self.chips, self.rows, self.width
        if kind in (XR, UR, HR, VR, YR, GR):
            return (r, w), BF16
        if kind in (FN, FS):
            return (c, 2 * r, w), BF16
        if kind == PREC:
            return (c, r, w), F32
        if kind == PART:
            return (c, 2 * r, w), F32
        if kind in (RFU, RFD, SA, SB):
            return (r // 2, w), F32
        if kind in (RU, RD):
            return (r, w), F32
        if kind in (QKV, DQKV):
            return (c, 2 * r, self.qkv_w), BF16
        if kind == MIX:
            return (c, 2 * r, self.mix_w), BF16
        if kind == LSE:
            return (c, self.mix_w // HEAD, 2 * r), F32
        if kind in (GP, GSUM):
            return (2 * self.layers, w), F32
        if kind == GBUF:
            return (self.count, 2 * self.layers, w), F32
        if kind in (GA, GM):
            return (1, w), F32
        if kind in (DK, DV):
            return (2 * c * r, HEAD), F32
        dims = {WQ: (w, self.qkv_w), WO: (self.mix_w, w), W1: (w, self.ff), W3: (w, self.ff), W2: (self.ff, w)}
        for group, dtype in (((WQ, WO, W1, W3, W2), BF16), ((AQ, AO, A1, A3, A2), F32), ((BQ, BO, B1, B3, B2), BF16)):
            if kind in group:
                return dims[WQ + group.index(kind)], dtype
        raise ValueError(kind)

    def comm_of(self, m, k):
        top = 2 * self.layers
        if k == 0:
            return None, None, None, None, None, None, None, ((UR, m, 0, FS),)
        if k < top:
            l = k // 2
            if k % 2:
                return 0, (XR, m, l), None, (GM, l), (HR, m, l), (VR, m, l), None, ()
            return 0, (HR, m, l - 1), None, (GA, l), (XR, m, l), (UR, m, l), None, ()
        if k == top:
            l = self.layers - 1
            return 1, (HR, m, l), None, None, (YR, m), None, None, ((VR, m, l, FS),)
        j = k - top
        l = self.layers - 1 - (j - 1) // 2
        if j % 2:
            return 2, (GR, m), (HR, m, l), (GM, l), (GR, m), None, self.layers + l, ((UR, m, l, FS),)
        sv = () if k == self.steps else ((VR, m, l - 1, FS),)
        return 2, (GR, m), (XR, m, l), (GA, l), (GR, m), None, l, sv

    def comp_of(self, m, k):
        top = 2 * self.layers
        if k < top:
            return (k % 2), k // 2
        return 2 + (k - top) % 2, self.layers - 1 - (k - top) // 2

    def products(self, n):
        if n == 0 or self.seq[n - 1][1] == self.steps:
            return None
        m, k = self.seq[n - 1]
        return (m, k) + self.comp_of(m, k)

    def uses(self, n):
        m, k = self.seq[n]
        ops = []
        kind, base, srow, gain, new, norm, slot, saved = self.comm_of(m, k)
        reads = [sv[:3] for sv in saved]
        writes = [(sv[3], m) for sv in saved]
        if kind is not None:
            reads += [(PREC, m), (RFU, m), (RFD, m), base] + [x for x in (srow, gain) if x]
            if slot is not None:
                reads.append((GP,))
                writes.append((GP,))
            writes += [x for x in (new, norm) if x]
            if kind == 1:
                reads.append((GR, m))
            if k < self.steps:
                writes.append((FN, m))
        if self.products(n):
            pm, pk, comp, l = self.products(n)
            reads += [(FS, pm)] if (comp >= 2 or pk == 0) else [(FN, pm)]
            reads += [(WQ, l), (WO, l)] if comp in (0, 3) else [(W1, l), (W3, l), (W2, l)]
            if comp >= 2:
                reads.append((FN, pm))
                acc = [(AQ,), (AO,)] if comp == 3 else [(A1,), (A3,), (A2,)]
                if pm > 0:
                    reads += acc
                writes += acc
            if comp == 3:
                reads += [(QKV, pm, l), (MIX, pm, l), (LSE, pm, l)]
            if comp == 0:
                writes += [(QKV, pm, l), (MIX, pm, l), (LSE, pm, l)]
            writes += [(PREC, pm), (RFU, pm), (RFD, pm)]
        return reads, writes

    def scratch(self, n):
        m, k = self.seq[n]
        kind = self.comm_of(m, k)[0]
        keys = []
        if kind is not None:
            keys += [(x, m) for x in (RU, RD, SA, SB)]
        if self.products(n):
            comp = self.products(n)[2]
            keys.append((PART,))
            if comp == 3:
                keys += [(DQKV,), (DK,), (DV,), (BQ,), (BO,)]
            if comp == 2:
                keys += [(B1,), (B3,), (B2,)]
        if n == len(self.seq) - 1:
            keys += [(GBUF,), (GSUM,)]
        return keys


class Kernel:
    def __init__(self, plan, cid, first, last):
        self.plan, self.cid, self.first, self.last = plan, cid, first, last
        written, self.live_in, keys = set(), [], []
        for n in range(first, last):
            reads, writes = plan.uses(n)
            for key in reads:
                if key not in written and key not in self.live_in and key != (GP,):
                    self.live_in.append(key)
            if (GP,) in reads and (GP,) not in written and n > 0 and any((GP,) in plan.uses(q)[1] for q in range(first)):
                if (GP,) not in self.live_in:
                    self.live_in.append((GP,))
            written |= set(writes)
            for key in reads + writes + plan.scratch(n):
                if key not in keys:
                    keys.append(key)
        later, seen = [], set()
        for n in range(last, len(plan.seq)):
            reads, writes = plan.uses(n)
            later += [key for key in reads if key in written and key not in seen and key not in later]
            seen |= set(writes)
        self.keys, self.live_out = keys, later
        self.zero_gp = (GP,) in keys and (GP,) not in self.live_in
        self.results = []
        for n in range(first, last):
            m, k = plan.seq[n]
            if k == 2 * plan.layers:
                self.results.append((YR, m))
            if k == plan.steps:
                self.results.append((GR, m))
            if plan.products(n):
                pm, pk, comp, l = plan.products(n)
                if pm == plan.micro - 1 and comp >= 2:
                    self.results += [(x, l) for x in ((BQ, BO) if comp == 3 else (B1, B3, B2))]
            if n == len(plan.seq) - 1:
                self.results.append((GSUM,))

    def out_shape(self, key):
        return jax.ShapeDtypeStruct(*self.plan.shape(key))

    def body(self, *refs):
        pn = self.plan
        ni, no, lo_ = len(self.live_in), len(self.live_out), len(self.results)
        ins = dict(zip(self.live_in, refs[:ni]))
        outs = dict(zip(self.live_out, refs[ni:ni + no]))
        res = dict(zip(self.results, refs[ni + no:ni + no + lo_]))
        s = dict(zip(self.keys, refs[ni + no + lo_:-5]))
        lsem, ssem, rsem, psem, qsem = refs[-5:]
        rows, chips, count = pn.rows, pn.chips, pn.count
        me = lax.axis_index('tp')
        chip, core = lax.div(me, 2), lax.rem(me, 2)
        oc = 1 - core
        cu, cd, cf = lax.rem(chip + 1, chips), lax.rem(chip + chips - 1, chips), lax.rem(chip + 2, chips)
        up, dn, sib = cu * 2 + core, cd * 2 + core, chip * 2 + oc
        final = self.last == len(pn.seq)
        nloc = [0]
        sent = [[] for _ in range(pn.micro)]

        def local(a, b):
            d = pltpu.make_async_copy(a, b, lsem.at[nloc[0]])
            nloc[0] += 1
            d.start()
            return d

        def remote(a, b, dev, m, slot, keep=True):
            d = pltpu.make_async_remote_copy(src_ref=a, dst_ref=b, send_sem=ssem.at[m, slot], recv_sem=rsem.at[m, slot],
                                             device_id={'tp': dev}, device_id_type=MESH)
            if keep:
                sent[m].append(d)
            return d

        def blk(ref, c, k, lo=0, size=rows):
            return ref.at[c, pl.ds(pl.multiple_of(k * rows + lo, 16), size)]

        barrier = pltpu.get_barrier_semaphore()
        peers = [lax.rem(me + off, count) for off in range(1, count)] if final else [up, dn, sib]
        for dev in peers:
            pl.semaphore_signal(barrier, inc=1, device_id={'tp': dev}, device_id_type=MESH)
        loads = {key: local(ins[key], s[key]) for key in self.live_in}
        stores = {}

        def need(*keys):
            for key in keys:
                if key in loads:
                    loads.pop(key).wait()

        def store(key, src, dst):
            stores[key] = local(src, dst)

        if self.zero_gp:
            s[(GP,)][...] = jnp.zeros_like(s[(GP,)])
        pl.semaphore_wait(barrier, len(peers))

        h2, h4 = rows // 2, rows // 4
        halves = range(2)
        far = [None] * pn.micro
        open_gathers = []

        def rs_far(m):
            red = s[(PREC, m)]
            far[m] = []
            for h in halves:
                lo = h * h2
                far[m].append((remote(red.at[cf, pl.ds(lo, h4)], s[(RFU, m)].at[pl.ds(h * h4, h4)], up, m, 4 * h, False),
                               remote(red.at[cf, pl.ds(lo + h4, h4)], s[(RFD, m)].at[pl.ds(h * h4, h4)], dn, m, 4 * h + 1, False)))
                for d in far[m][h]:
                    d.start()

        def rs_mid(m):
            need((PREC, m), (RFU, m), (RFD, m))
            red, dep, ind = s[(PREC, m)], [], []
            for h in halves:
                lo, q = h * h2, pl.ds(h * h4, h4)
                if far[m]:
                    for d in far[m][h]:
                        d.wait_recv()
                s[(SA, m)][q] = red[cu, pl.ds(lo, h4)] + s[(RFU, m)][q]
                s[(SB, m)][q] = red[cd, pl.ds(lo + h4, h4)] + s[(RFD, m)][q]
                dep.append((remote(s[(SA, m)].at[q], s[(RU, m)].at[pl.ds(lo, h4)], up, m, 4 * h + 2),
                            remote(s[(SB, m)].at[q], s[(RD, m)].at[pl.ds(lo + h4, h4)], dn, m, 4 * h + 3)))
                for d in dep[h]:
                    d.start()
            drain = [d for pair in far[m] or [] for d in pair]
            far[m] = None
            for h in halves:
                lo = h * h2
                ind.append((remote(red.at[cu, pl.ds(lo + h4, h4)], s[(RU, m)].at[pl.ds(lo + h4, h4)], up, m, 8 + 2 * h, False),
                            remote(red.at[cd, pl.ds(lo, h4)], s[(RD, m)].at[pl.ds(lo, h4)], dn, m, 9 + 2 * h, False)))
                for d in ind[h]:
                    d.start()
            return [dep[h] + ind[h] for h in halves], drain + [d for pair in ind for d in pair]

        def ag_make(full, m, lo, size, slot):
            own = blk(full, chip, core, lo, size)
            return [remote(own, own, up, m, slot), remote(own, own, dn, m, slot + 1), remote(own, own, sib, m, slot + 2)]

        def ag_mid(full, m, lo, size, slot, st):
            a = size // 2
            st[0].wait_recv()
            fa = blk(full, cd, core, lo, a)
            st.append(remote(fa, fa, up, m, slot + 3))
            st[3].start()
            st[1].wait_recv()
            fb = blk(full, cu, core, lo + a, a)
            st.append(remote(fb, fb, dn, m, slot + 4))
            st[4].start()
            for q, c in enumerate((cd, cu)):
                r = blk(full, c, core, lo, size)
                st.append(remote(r, r, sib, m, slot + 5 + q))
                st[5 + q].start()

        def ag_far(full, m, lo, size, slot, st):
            st[3].wait_recv()
            st[4].wait_recv()
            r = blk(full, cf, core, lo, size)
            st.append(remote(r, r, sib, m, slot + 7))
            st[7].start()

        def ag_end(full, m, lo, size, slot, st):
            for q in (2, 5, 6, 7):
                st[q].wait_recv()

        def close():
            for g in open_gathers:
                ag_far(*g)
            for g in open_gathers:
                ag_end(*g)
            for g in open_gathers:
                for d in sent[g[1]]:
                    d.wait_send()
                sent[g[1]].clear()
            open_gathers.clear()

        def part_copy(m, t):
            return pltpu.make_async_remote_copy(
                src_ref=s[(PART,)].at[t, pl.ds(pl.multiple_of(oc * rows, 16), rows)], dst_ref=s[(PREC, m)].at[t],
                send_sem=psem.at[m, t], recv_sem=qsem.at[m, t], device_id={'tp': sib}, device_id_type=MESH)

        def loop(fn, m=None, hook=None, at=0):
            def step(t, carry):
                fn(t)
                if m is not None:
                    @pl.when(t > 0)
                    def _():
                        part_copy(m, t - 1).start()
                if hook is not None:
                    @pl.when(t == at)
                    def _():
                        hook()
                return carry
            lax.fori_loop(0, chips, step, 0)
            if m is not None:
                part_copy(m, chips - 1).start()


        for n in range(self.first, self.last):
            m, k = pn.seq[n]
            kind, base, srow, gain, new, norm, slot, saved = pn.comm_of(m, k)
            gathers = []
            arrive, drain = rs_mid(m) if kind is not None else (None, None)
            for q, sv in enumerate(saved):
                key = sv[:3]
                need(key)
                full = s[(sv[3], m)]
                full[chip, pl.ds(pl.multiple_of(core * rows, 16), rows)] = s[key][...]
                st = ag_make(full, m, 0, rows, 12 + 8 * q)
                for d in st:
                    d.start()
                gathers.append((full, m, 0, rows, 12 + 8 * q, st))
            close()

            hook = None
            if kind is not None:
                need(*[x for x in (base, srow, gain) if x])
                if slot is not None:
                    need((GP,))
                news = []
                if kind == 1:
                    need((GR, m))
                if k < pn.steps:
                    full = s[(FN, m)]
                    news = [(full, m, h * h2, h2, 28 + 8 * h, ag_make(full, m, h * h2, h2, 28 + 8 * h)) for h in halves]
                starts = [pl.multiple_of(core * rows + h * h2, 16) for h in halves]
                hook = functools.partial(self.rows_step, s, m, kind, base, srow, gain, new, norm, slot, arrive, drain, news, starts, chip, h2)

            if pn.products(n):
                pm, pk, comp, l = pn.products(n)
                full = s[(FS, pm)] if (comp >= 2 or pk == 0) else s[(FN, pm)]
                need((FS, pm), (FN, pm))
                fn = (self.attn_f, self.mlp_f, self.mlp_b, self.attn_b)[comp]
                for x in ((BQ, BO) if comp == 3 else (B1, B3, B2) if comp == 2 else ()):
                    if (x, l + 1) in stores:
                        stores.pop((x, l + 1)).wait()
                fn(s, need, loop, hook, pm, l, full)
                red = s[(PREC, pm)]
                for c in range(chips):
                    d = part_copy(pm, c)
                    d.wait_recv()
                    red[c] = red[c] + s[(PART,)][c, pl.ds(pl.multiple_of(core * rows, 16), rows)]
                    d.wait_send()
                rs_far(pm)
                if comp >= 2 and pm == pn.micro - 1:
                    for a, b in ((AQ, BQ), (AO, BO)) if comp == 3 else ((A1, B1), (A3, B3), (A2, B2)):
                        s[(b,)][...] = s[(a,)][...].astype(BF16)
                        store((b, l), s[(b,)], res[(b, l)])
            elif hook is not None:
                hook()

            if kind is not None:
                gathers += news
            if new is not None and new in res and (new[0] == YR or k == pn.steps):
                store(new, s[new], res[new])
            for g in gathers:
                ag_mid(*g)
            open_gathers.extend(gathers)

        close()
        if final:
            gb = s[(GBUF,)]
            gb[me] = s[(GP,)][...]
            gs = [remote(gb.at[me], gb.at[me], lax.rem(me + off, count), 0, 43 + off) for off in range(1, count)]
            for d in gs:
                d.start()
            for d in gs:
                d.wait_recv()
            acc = gb[0]
            for q in range(1, count):
                acc = acc + gb[q]
            s[(GSUM,)][...] = acc
            store((GSUM,), s[(GSUM,)], res[(GSUM,)])
        for m in range(pn.micro):
            if far[m]:
                for pair in far[m]:
                    for d in pair:
                        d.wait_recv()
                        d.wait_send()
            for d in sent[m]:
                d.wait_send()
        for key in self.live_out:
            need(key)
            store((key,), s[key], outs[key])
        for d in stores.values():
            d.wait()
        assert not loads

    def rows_step(self, s, m, kind, base, srow, gain, new, norm, slot, arrive, drain, news, starts, chip, h2):
        red, ru, rd = s[(PREC, m)], s[(RU, m)], s[(RD, m)]
        for h in range(2):
            for d in arrive[h]:
                d.wait_recv()
            q = pl.ds(h * h2, h2)
            total = (red[chip, q] + ru[q] + rd[q]).astype(BF16).astype(F32)
            if kind == 2:
                x = s[srow][q].astype(F32)
                scale = lax.rsqrt(jnp.mean(x * x, axis=-1, keepdims=True) + NORM_EPS)
                s[(GP,)][slot:slot + 1] += jnp.sum(total * x * scale, axis=0, keepdims=True)
                ct = total * s[gain][...]
                total = scale * ct - x * (scale * scale * scale) * jnp.mean(ct * x, axis=-1, keepdims=True)
            val = (s[base][q].astype(F32) + total).astype(BF16)
            s[new][q] = val
            if kind == 0:
                val = norm_rows(val.astype(F32), s[gain][...]).astype(BF16)
                s[norm][q] = val
            if kind == 1:
                val = s[(GR, m)][q]
            if h == 1:
                for d in drain:
                    d.wait_send()
            if news:
                s[(FN, m)][chip, pl.ds(starts[h], h2)] = val
                for d in news[h][5]:
                    d.start()

    def scores(self, t, keys, q):
        total, rows2 = keys.shape[0], q.shape[0]
        sc = dot_nt(keys, q) * HEAD ** -0.5
        kpos = lax.broadcasted_iota(jnp.int32, (total, rows2), 0)
        qpos = lax.broadcasted_iota(jnp.int32, (total, rows2), 1) + t * rows2
        return jnp.where(kpos <= qpos, sc, -1e30)

    def heads(self, qkv):
        ow, total = self.plan.mix_w, 2 * self.plan.chips * self.plan.rows
        return (qkv[:, :, ow:ow + HEAD].reshape(total, HEAD), qkv[:, :, ow + HEAD:ow + 2 * HEAD].reshape(total, HEAD))

    def attn_f(self, s, need, loop, hook, m, l, full):
        need((WQ, l), (WO, l))
        qkv, mix, lse = s[(QKV, m, l)], s[(MIX, m, l)], s[(LSE, m, l)]

        def proj(t):
            qkv[t] = dot_nn(full[t], s[(WQ, l)][...]).astype(BF16)
        loop(proj)

        def attend(t):
            keys, vals = self.heads(qkv)
            for h in range(self.plan.mix_w // HEAD):
                cols = slice(h * HEAD, (h + 1) * HEAD)
                sc = self.scores(t, keys, qkv[t, :, cols])
                top = jnp.max(sc, axis=0, keepdims=True)
                ex = jnp.exp(sc - top)
                tot = jnp.sum(ex, axis=0, keepdims=True)
                lse[t, h:h + 1] = top + jnp.log(tot)
                mix[t, :, cols] = dot_tn((ex * (1.0 / tot)).astype(BF16), vals).astype(BF16)
            s[(PART,)][t] = dot_nn(mix[t], s[(WO, l)][...])
        loop(attend, m, hook, 1)

    def mlp_f(self, s, need, loop, hook, m, l, full):
        need((W1, l), (W3, l), (W2, l))

        def tile(t):
            v = full[t]
            g = dot_nn(v, s[(W1, l)][...])
            w = dot_nn(v, s[(W3, l)][...])
            s[(PART,)][t] = dot_nn((g * jax.nn.sigmoid(g) * w).astype(BF16), s[(W2, l)][...])
        loop(tile, m)
        if hook is not None:
            hook()

    def start_sums(self, s, need, m, keys):
        for key in keys:
            if m > 0:
                need(key)
            else:
                s[key][...] = jnp.zeros_like(s[key])

    def mlp_b(self, s, need, loop, hook, m, l, full):
        need((W1, l), (W3, l), (W2, l))
        self.start_sums(s, need, m, ((A1,), (A3,), (A2,)))
        grad = s[(FN, m)]

        def tile(t):
            v, dy = full[t], grad[t]
            g = dot_nn(v, s[(W1, l)][...])
            w = dot_nn(v, s[(W3, l)][...])
            sig = jax.nn.sigmoid(g)
            act = g * sig
            s[(A2,)][...] += dot_tn((act * w).astype(BF16), dy)
            dm = dot_nt(dy, s[(W2, l)][...]).astype(BF16).astype(F32)
            dw = (dm * act).astype(BF16)
            dg = (dm * w * sig * (1.0 + g * (1.0 - sig))).astype(BF16)
            s[(A1,)][...] += dot_tn(v, dg)
            s[(A3,)][...] += dot_tn(v, dw)
            s[(PART,)][t] = dot_nt(dg, s[(W1, l)][...]) + dot_nt(dw, s[(W3, l)][...])
        loop(tile, m, hook, 2)

    def attn_b(self, s, need, loop, hook, m, l, full):
        need((WQ, l), (WO, l), (QKV, m, l), (MIX, m, l), (LSE, m, l))
        self.start_sums(s, need, m, ((AQ,), (AO,)))
        grad, dqkv, dk, dv = s[(FN, m)], s[(DQKV,)], s[(DK,)], s[(DV,)]
        qkv, mix, lse = s[(QKV, m, l)], s[(MIX, m, l)], s[(LSE, m, l)]
        dk[...] = jnp.zeros_like(dk)
        dv[...] = jnp.zeros_like(dv)

        def attend(t):
            dh = grad[t]
            s[(AO,)][...] += dot_tn(mix[t], dh)
            do = dot_nt(dh, s[(WO, l)][...]).astype(BF16)
            keys, vals = self.heads(qkv)
            for h in range(self.plan.mix_w // HEAD):
                cols = slice(h * HEAD, (h + 1) * HEAD)
                q, doh = qkv[t, :, cols], do[:, cols]
                prob = jnp.exp(self.scores(t, keys, q) - lse[t, h:h + 1])
                dv[...] += dot_nn(prob.astype(BF16), doh)
                dp = dot_nt(vals, doh).astype(BF16).astype(F32)
                rd = jnp.sum(dp * prob, axis=0, keepdims=True)
                ds = (prob * (dp - rd) * HEAD ** -0.5).astype(BF16)
                dk[...] += dot_nn(ds, q)
                dqkv[t, :, cols] = dot_tn(ds, keys).astype(BF16)
        loop(attend, None, hook, 2)
        ow, shp = self.plan.mix_w, dqkv.shape[:2] + (HEAD,)
        dqkv[:, :, ow:ow + HEAD] = dk[...].astype(BF16).reshape(shp)
        dqkv[:, :, ow + HEAD:ow + 2 * HEAD] = dv[...].astype(BF16).reshape(shp)

        def tile(t):
            s[(AQ,)][...] += dot_tn(full[t], dqkv[t])
            s[(PART,)][t] = dot_nt(dqkv[t], s[(WQ, l)][...])
        loop(tile, m)

    def run(self, state):
        any_spec = pl.BlockSpec(memory_space=pl.ANY)
        out_keys = self.live_out + self.results
        pn = self.plan
        vals = pl.pallas_call(
            self.body,
            out_shape=[self.out_shape((key[0],)) if key[0] in (BQ, BO, B1, B3, B2) else self.out_shape(key) for key in out_keys],
            in_specs=[any_spec] * len(self.live_in),
            out_specs=[any_spec] * len(out_keys),
            scratch_shapes=[pltpu.VMEM(*pn.shape(key)) for key in self.keys] + [
                pltpu.SemaphoreType.DMA((len(self.live_in) + len(out_keys),)),
                pltpu.SemaphoreType.DMA((pn.micro, 52)), pltpu.SemaphoreType.DMA((pn.micro, 52)),
                pltpu.SemaphoreType.DMA((pn.micro, pn.chips)), pltpu.SemaphoreType.DMA((pn.micro, pn.chips))],
            compiler_params=pltpu.CompilerParams(collective_id=self.cid, has_side_effects=True, vmem_limit_bytes=VMEM_BYTES),
        )(*[state[key] for key in self.live_in])
        state.update(zip(out_keys, vals))


def solution(mesh):
    rows_p = P(None, ('dp', 'tp'), None)
    flat = P(None, None)
    cols_p = P(None, None, 'tp')
    head_p = P(None, 'tp', None, None)
    down_p = P(None, 'tp', None)
    count = mesh.shape['tp']

    def device_program(x_in, y_cot, gain_attn, gain_mlp, w_qkv, w_out, w_gate, w_up, w_down):
        micro, rows, width = x_in.shape
        layers = w_qkv.shape[0]
        wq = w_qkv.reshape(layers, width, -1)
        wo = w_out.reshape(layers, -1, width)
        plan = Plan(count, micro, layers, rows, width, wq.shape[2], wo.shape[1], w_gate.shape[2])
        state = {}
        for m in range(micro):
            state[(XR, m, 0)] = x_in[m]
            state[(GR, m)] = y_cot[m]
            state[(UR, m, 0)] = norm_rows(x_in[m].astype(F32), gain_attn[0:1]).astype(BF16)
        for l in range(layers):
            for key, arr in ((WQ, wq), (WO, wo), (W1, w_gate), (W3, w_up), (W2, w_down)):
                state[(key, l)] = arr[l]
            state[(GA, l)], state[(GM, l)] = gain_attn[l:l + 1], gain_mlp[l:l + 1]
        cuts = [0] + list(SPLITS) + [len(plan.seq)]
        for cid in range(len(cuts) - 1):
            Kernel(plan, cid, cuts[cid], cuts[cid + 1]).run(state)

        def stack(key, shape):
            return jnp.stack([state[(key, l)].reshape(shape) for l in range(layers)])

        gsum = state[(GSUM,)]
        return (jnp.stack([state[(YR, m)] for m in range(micro)]), jnp.stack([state[(GR, m)] for m in range(micro)]),
                stack(BQ, w_qkv.shape[1:]), stack(BO, w_out.shape[1:]), stack(B1, w_gate.shape[1:]),
                stack(B3, w_up.shape[1:]), stack(B2, w_down.shape[1:]), gsum[:layers], gsum[layers:])

    return jax.shard_map(device_program, mesh=mesh,
                         in_specs=(rows_p, rows_p, flat, flat, P(None, None, 'tp', None, None), head_p, cols_p, cols_p, down_p),
                         out_specs=(rows_p, rows_p, P('dp', None, 'tp', None, None), P('dp', 'tp', None, None), P('dp', None, 'tp'),
                                    P('dp', None, 'tp'), P('dp', 'tp', None), P('dp', None), P('dp', None)),
                         check_vma=False)
```

```python
import functools

import jax
import jax.numpy as jnp
from jax import lax
from jax.experimental import pallas as pl
from jax.experimental.pallas import tpu as pltpu
from jax.sharding import PartitionSpec as P

NORM_EPS = 1e-5
MESH = pl.DeviceIdType.MESH
BF16 = jnp.bfloat16
F32 = jnp.float32
VMEM_BYTES = 67043328
HEAD = 128
SPLITS = ()

(XR, UR, HR, VR, YR, GR, FN, FS, PREC, RFU, RFD, RU, RD, SA, SB, QKV, MIX, LSE, GP,
 WQ, WO, W1, W3, W2, GA, GM, AQ, AO, A1, A3, A2, BQ, BO, B1, B3, B2, PART, DQKV, DK, DV, GBUF, GSUM) = range(42)


def dot_nn(a, b):
    return lax.dot_general(a, b, (((1,), (0,)), ((), ())), preferred_element_type=F32)


def dot_nt(a, b):
    return lax.dot_general(a, b, (((1,), (1,)), ((), ())), preferred_element_type=F32)


def dot_tn(a, b):
    return lax.dot_general(a, b, (((0,), (0,)), ((), ())), preferred_element_type=F32)


def norm_rows(rows, gain):
    return rows * lax.rsqrt(jnp.mean(rows * rows, axis=-1, keepdims=True) + NORM_EPS) * gain


class Plan:
    def __init__(self, count, micro, layers, rows, width, qkv_w, mix_w, ff):
        self.count, self.micro, self.layers, self.rows, self.width = count, micro, layers, rows, width
        self.qkv_w, self.mix_w, self.ff = qkv_w, mix_w, ff
        self.chips = count // 2
        self.steps = 4 * layers
        self.seq = [(m, k) for k in range(self.steps + 1) for m in range(micro)]

    def shape(self, key):
        kind = key[0]
        c, r, w = self.chips, self.rows, self.width
        if kind in (XR, UR, HR, VR, YR, GR):
            return (r, w), BF16
        if kind in (FN, FS):
            return (c, 2 * r, w), BF16
        if kind == PREC:
            return (c, r, w), F32
        if kind == PART:
            return (c, 2 * r, w), F32
        if kind in (RFU, RFD, SA, SB):
            return (r // 2, w), F32
        if kind in (RU, RD):
            return (r, w), F32
        if kind in (QKV, DQKV):
            return (c, 2 * r, self.qkv_w), BF16
        if kind == MIX:
            return (c, 2 * r, self.mix_w), BF16
        if kind == LSE:
            return (c, self.mix_w // HEAD, 2 * r), F32
        if kind in (GP, GSUM):
            return (2 * self.layers, w), F32
        if kind == GBUF:
            return (self.count, 2 * self.layers, w), F32
        if kind in (GA, GM):
            return (self.layers, w), F32
        if kind in (DK, DV):
            return (2 * c * r, HEAD), F32
        dims = {WQ: (w, self.qkv_w), WO: (self.mix_w, w), W1: (w, self.ff), W3: (w, self.ff), W2: (self.ff, w)}
        for group, dtype in (((WQ, WO, W1, W3, W2), BF16), ((AQ, AO, A1, A3, A2), F32), ((BQ, BO, B1, B3, B2), BF16)):
            if kind in group:
                return dims[WQ + group.index(kind)], dtype
        raise ValueError(kind)

    def comm_of(self, m, k):
        top = 2 * self.layers
        if k == 0:
            return None, None, None, None, None, None, None, ((UR, m, 0, FS),)
        if k < top:
            l = k // 2
            if k % 2:
                return 0, (XR, m, l), None, (GM, l), (HR, m, l), (VR, m, l), None, ()
            return 0, (HR, m, l - 1), None, (GA, l), (XR, m, l), (UR, m, l), None, ()
        if k == top:
            l = self.layers - 1
            return 1, (HR, m, l), None, None, (YR, m), None, None, ((VR, m, l, FS),)
        j = k - top
        l = self.layers - 1 - (j - 1) // 2
        if j % 2:
            return 2, (GR, m), (HR, m, l), (GM, l), (GR, m), None, self.layers + l, ((UR, m, l, FS),)
        sv = () if k == self.steps else ((VR, m, l - 1, FS),)
        return 2, (GR, m), (XR, m, l), (GA, l), (GR, m), None, l, sv

    def comp_of(self, m, k):
        top = 2 * self.layers
        if k < top:
            return (k % 2), k // 2
        return 2 + (k - top) % 2, self.layers - 1 - (k - top) // 2

    def products(self, n):
        if n == 0 or self.seq[n - 1][1] == self.steps:
            return None
        m, k = self.seq[n - 1]
        return (m, k) + self.comp_of(m, k)

    def uses(self, n):
        m, k = self.seq[n]
        ops = []
        kind, base, srow, gain, new, norm, slot, saved = self.comm_of(m, k)
        reads = [sv[:3] for sv in saved] if k else [(XR, m, 0), (GA,)]
        writes = [(sv[3], m) for sv in saved] + ([] if k else [(UR, m, 0)])
        if kind is not None:
            reads += [(PREC, m), (RFU, m), (RFD, m), base] + [x for x in (srow, gain and gain[:1]) if x]
            if slot is not None:
                reads.append((GP,))
                writes.append((GP,))
            writes += [x for x in (new, norm) if x]
            if kind == 1:
                reads.append((GR, m))
            if k < self.steps:
                writes.append((FN, m))
        if self.products(n):
            pm, pk, comp, l = self.products(n)
            reads += [(FS, pm)] if (comp >= 2 or pk == 0) else [(FN, pm)]
            reads += [(WQ, l), (WO, l)] if comp in (0, 3) else [(W1, l), (W3, l), (W2, l)]
            if comp >= 2:
                reads.append((FN, pm))
                acc = [(AQ,), (AO,)] if comp == 3 else [(A1,), (A3,), (A2,)]
                if pm > 0:
                    reads += acc
                writes += acc
            if comp == 3:
                reads += [(QKV, pm, l), (MIX, pm, l), (LSE, pm, l)]
            if comp == 0:
                writes += [(QKV, pm, l), (MIX, pm, l), (LSE, pm, l)]
            writes += [(PREC, pm), (RFU, pm), (RFD, pm)]
        return reads, writes

    def scratch(self, n):
        m, k = self.seq[n]
        kind = self.comm_of(m, k)[0]
        keys = []
        if kind is not None:
            keys += [(x, m) for x in (RU, RD, SA, SB)]
        if self.products(n):
            comp = self.products(n)[2]
            keys.append((PART,))
            if comp == 3:
                keys += [(DQKV,), (DK,), (DV,), (BQ,), (BO,)]
            if comp == 2:
                keys += [(B1,), (B3,), (B2,)]
        if n == len(self.seq) - 1:
            keys += [(GBUF,), (GSUM,)]
        return keys


class Kernel:
    def __init__(self, plan, cid, first, last):
        self.plan, self.cid, self.first, self.last = plan, cid, first, last
        written, self.live_in, keys = set(), [], []
        for n in range(first, last):
            reads, writes = plan.uses(n)
            for key in reads:
                if key not in written and key not in self.live_in and key != (GP,):
                    self.live_in.append(key)
            if (GP,) in reads and (GP,) not in written and n > 0 and any((GP,) in plan.uses(q)[1] for q in range(first)):
                if (GP,) not in self.live_in:
                    self.live_in.append((GP,))
            written |= set(writes)
            for key in reads + writes + plan.scratch(n):
                if key not in keys:
                    keys.append(key)
        later, seen = [], set()
        for n in range(last, len(plan.seq)):
            reads, writes = plan.uses(n)
            later += [key for key in reads if key in written and key not in seen and key not in later]
            seen |= set(writes)
        self.keys, self.live_out = keys, later
        self.zero_gp = (GP,) in keys and (GP,) not in self.live_in
        self.results = []
        for n in range(first, last):
            m, k = plan.seq[n]
            if k == 2 * plan.layers:
                self.results.append((YR, m))
            if k == plan.steps:
                self.results.append((GR, m))
            if plan.products(n):
                pm, pk, comp, l = plan.products(n)
                if pm == plan.micro - 1 and comp >= 2:
                    self.results += [(x, l) for x in ((BQ, BO) if comp == 3 else (B1, B3, B2))]
            if n == len(plan.seq) - 1:
                self.results.append((GSUM,))

    def out_shape(self, key):
        return jax.ShapeDtypeStruct(*self.plan.shape(key))

    def body(self, *refs):
        pn = self.plan
        ni, no, lo_ = len(self.arrays), len(self.live_out), len(self.stacks)
        ins = {}
        for key in self.live_in:
            q, idx = self.place[key]
            ins[key] = refs[q] if idx is None else refs[q].at[idx]
        outs = dict(zip(self.live_out, refs[ni:ni + no]))
        piles = dict(zip(self.stacks, refs[ni + no:ni + no + lo_]))
        res = {key: piles[key[:1]] if len(key) == 1 else piles[key[:1]].at[key[1]] for key in self.results}
        s = dict(zip(self.keys, refs[ni + no + lo_:-5]))
        lsem, ssem, rsem, psem, qsem = refs[-5:]
        rows, chips, count = pn.rows, pn.chips, pn.count
        me = lax.axis_index('tp')
        chip, core = lax.div(me, 2), lax.rem(me, 2)
        oc = 1 - core
        cu, cd, cf = lax.rem(chip + 1, chips), lax.rem(chip + chips - 1, chips), lax.rem(chip + 2, chips)
        up, dn, sib = cu * 2 + core, cd * 2 + core, chip * 2 + oc
        final = self.last == len(pn.seq)
        nloc = [0]
        sent = [[] for _ in range(pn.micro)]

        def local(a, b):
            d = pltpu.make_async_copy(a, b, lsem.at[nloc[0]])
            nloc[0] += 1
            d.start()
            return d

        def remote(a, b, dev, m, slot, keep=True):
            d = pltpu.make_async_remote_copy(src_ref=a, dst_ref=b, send_sem=ssem.at[m, slot], recv_sem=rsem.at[m, slot],
                                             device_id={'tp': dev}, device_id_type=MESH)
            if keep:
                sent[m].append(d)
            return d

        def blk(ref, c, k, lo=0, size=rows):
            return ref.at[c, pl.ds(pl.multiple_of(k * rows + lo, 16), size)]

        barrier = pltpu.get_barrier_semaphore()
        peers = [lax.rem(me + off, count) for off in range(1, count)] if final else [up, dn, sib]
        for dev in peers:
            pl.semaphore_signal(barrier, inc=1, device_id={'tp': dev}, device_id_type=MESH)
        loads = {key: local(ins[key], s[key]) for key in self.live_in}
        stores = {}

        def need(*keys):
            for key in keys:
                if key in loads:
                    loads.pop(key).wait()

        def store(key, src, dst):
            stores[key] = local(src, dst)

        if self.zero_gp:
            s[(GP,)][...] = jnp.zeros_like(s[(GP,)])
        pl.semaphore_wait(barrier, len(peers))

        h2, h4 = rows // 2, rows // 4
        halves = range(2)
        far = [None] * pn.micro
        open_gathers = []

        def rs_far(m):
            red = s[(PREC, m)]
            far[m] = []
            for h in halves:
                lo = h * h2
                far[m].append((remote(red.at[cf, pl.ds(lo, h4)], s[(RFU, m)].at[pl.ds(h * h4, h4)], up, m, 4 * h, False),
                               remote(red.at[cf, pl.ds(lo + h4, h4)], s[(RFD, m)].at[pl.ds(h * h4, h4)], dn, m, 4 * h + 1, False)))

        def fold(m, c):
            d = part_copy(m, c)
            d.wait_recv()
            s[(PREC, m)][c] = s[(PREC, m)][c] + s[(PART,)][c, pl.ds(pl.multiple_of(core * rows, 16), rows)]
            d.wait_send()

        def fold_far(m):
            fold(m, cf)
            for pair in far[m]:
                for d in pair:
                    d.start()

        def rs_mid(m):
            need((PREC, m), (RFU, m), (RFD, m))
            red, dep, ind = s[(PREC, m)], [], []
            for h in halves:
                lo, q = h * h2, pl.ds(h * h4, h4)
                if far[m]:
                    for d in far[m][h]:
                        d.wait_recv()
                s[(SA, m)][q] = red[cu, pl.ds(lo, h4)] + s[(RFU, m)][q]
                s[(SB, m)][q] = red[cd, pl.ds(lo + h4, h4)] + s[(RFD, m)][q]
                dep.append((remote(s[(SA, m)].at[q], s[(RU, m)].at[pl.ds(lo, h4)], up, m, 4 * h + 2),
                            remote(s[(SB, m)].at[q], s[(RD, m)].at[pl.ds(lo + h4, h4)], dn, m, 4 * h + 3)))
                for d in dep[h]:
                    d.start()
            drain = [d for pair in far[m] or [] for d in pair]
            far[m] = None
            for h in halves:
                lo = h * h2
                ind.append((remote(red.at[cu, pl.ds(lo + h4, h4)], s[(RU, m)].at[pl.ds(lo + h4, h4)], up, m, 8 + 2 * h, False),
                            remote(red.at[cd, pl.ds(lo, h4)], s[(RD, m)].at[pl.ds(lo, h4)], dn, m, 9 + 2 * h, False)))
                for d in ind[h]:
                    d.start()
            return [dep[h] + ind[h] for h in halves], drain + [d for pair in ind for d in pair]

        def ag_make(full, m, lo, size, slot):
            own = blk(full, chip, core, lo, size)
            return [remote(own, own, up, m, slot), remote(own, own, dn, m, slot + 1), remote(own, own, sib, m, slot + 2)]

        def ag_mid(full, m, lo, size, slot, st):
            a = size // 2
            st[0].wait_recv()
            fa = blk(full, cd, core, lo, a)
            st.append(remote(fa, fa, up, m, slot + 3))
            st[3].start()
            st[1].wait_recv()
            fb = blk(full, cu, core, lo + a, a)
            st.append(remote(fb, fb, dn, m, slot + 4))
            st[4].start()
            for q, c in enumerate((cd, cu)):
                r = blk(full, c, core, lo, size)
                st.append(remote(r, r, sib, m, slot + 5 + q))
                st[5 + q].start()

        def ag_far(full, m, lo, size, slot, st):
            st[3].wait_recv()
            st[4].wait_recv()
            r = blk(full, cf, core, lo, size)
            st.append(remote(r, r, sib, m, slot + 7))
            st[7].start()

        def ag_end(full, m, lo, size, slot, st):
            for q in (2, 5, 6, 7):
                st[q].wait_recv()

        def close():
            for g in open_gathers:
                ag_far(*g)
            for g in open_gathers:
                ag_end(*g)
            for g in open_gathers:
                for d in sent[g[1]]:
                    d.wait_send()
                sent[g[1]].clear()
            open_gathers.clear()

        def part_copy(m, t):
            return pltpu.make_async_remote_copy(
                src_ref=s[(PART,)].at[t, pl.ds(pl.multiple_of(oc * rows, 16), rows)], dst_ref=s[(PREC, m)].at[t],
                send_sem=psem.at[m, t], recv_sem=qsem.at[m, t], device_id={'tp': sib}, device_id_type=MESH)

        def loop(fn, m=None, hook=None, at=0, lo=0, hi=chips, spin=False):
            def tile(t):
                return lax.rem(chip + 2 + 3 * t, chips) if spin else t

            def step(t, carry):
                fn(tile(t))
                if m is not None:
                    @pl.when(t > 0)
                    def _():
                        part_copy(m, tile(t - 1)).start()
                if hook is not None:
                    @pl.when(t == at)
                    def _():
                        hook()
                return carry
            lax.fori_loop(lo, hi, step, 0)
            if m is not None and hi == chips:
                part_copy(m, tile(chips - 1)).start()


        for n in range(self.first, self.last):
            m, k = pn.seq[n]
            kind, base, srow, gain, new, norm, slot, saved = pn.comm_of(m, k)
            gathers = []
            arrive, drain = rs_mid(m) if kind is not None else (None, None)
            for q, sv in enumerate(saved):
                key = sv[:3]
                need(key)
                if k == 0:
                    need((XR, m, 0), (GA,))
                    s[key][...] = norm_rows(s[(XR, m, 0)][...].astype(F32), s[(GA,)][0:1]).astype(BF16)
                full = s[(sv[3], m)]
                full[chip, pl.ds(pl.multiple_of(core * rows, 16), rows)] = s[key][...]
                cut = [(0, rows, 12 + 8 * q)] if k else [(h * h2, h2, 28 + 8 * h) for h in halves]
                for lo, size, first in cut:
                    st = ag_make(full, m, lo, size, first)
                    for d in st:
                        d.start()
                    gathers.append((full, m, lo, size, first, st))
            close()

            hook = None
            if kind is not None:
                need(*[x for x in (base, srow, gain and gain[:1]) if x])
                if slot is not None:
                    need((GP,))
                news = []
                if kind == 1:
                    need((GR, m))
                if k < pn.steps:
                    full = s[(FN, m)]
                    news = [(full, m, h * h2, h2, 28 + 8 * h, ag_make(full, m, h * h2, h2, 28 + 8 * h)) for h in halves]
                starts = [pl.multiple_of(core * rows + h * h2, 16) for h in halves]
                hook = functools.partial(self.rows_step, s, m, kind, base, srow, gain, new, norm, slot, arrive, drain, news, starts, chip, h2)

            if pn.products(n):
                pm, pk, comp, l = pn.products(n)
                full = s[(FS, pm)] if (comp >= 2 or pk == 0) else s[(FN, pm)]
                need((FS, pm), (FN, pm))
                fn = (self.attn_f, self.mlp_f, self.mlp_b, self.attn_b)[comp]
                for x in ((BQ, BO) if comp == 3 else (B1, B3, B2) if comp == 2 else ()):
                    if (x, l + 1) in stores:
                        stores.pop((x, l + 1)).wait()
                rs_far(pm)
                early = functools.partial(fold_far, pm)
                late = fn(s, need, loop, hook, pm, l, full, early, n == 1 or n == len(pn.seq) - 2)
                if comp != 3 or l:
                    early()
                for c in (cu, cd, chip):
                    fold(pm, c)
                if late is not None:
                    late()
                if comp >= 2 and pm == pn.micro - 1:
                    for a, b in ((AQ, BQ), (AO, BO)) if comp == 3 else ((A1, B1), (A3, B3), (A2, B2)):
                        s[(b,)][...] = s[(a,)][...].astype(BF16)
                        store((b, l), s[(b,)], res[(b, l)])
            elif hook is not None:
                hook()

            if kind is not None:
                gathers += news
            if new is not None and new in res and (new[0] == YR or k == pn.steps):
                store(new, s[new], res[new])
            for g in gathers:
                ag_mid(*g)
            open_gathers.extend(gathers)

        close()
        if final:
            gb = s[(GBUF,)]
            gb[me] = s[(GP,)][...]
            gs = [remote(gb.at[me], gb.at[me], lax.rem(me + off, count), 0, 43 + off) for off in range(1, count)]
            for d in gs:
                d.start()
            for d in gs:
                d.wait_recv()
            acc = gb[0]
            for q in range(1, count):
                acc = acc + gb[q]
            s[(GSUM,)][...] = acc
            store((GSUM,), s[(GSUM,)], res[(GSUM,)])
        for m in range(pn.micro):
            if far[m]:
                for pair in far[m]:
                    for d in pair:
                        d.wait_recv()
                        d.wait_send()
            for d in sent[m]:
                d.wait_send()
        for key in self.live_out:
            need(key)
            store((key,), s[key], outs[key])
        for d in stores.values():
            d.wait()
        assert not loads

    def rows_step(self, s, m, kind, base, srow, gain, new, norm, slot, arrive, drain, news, starts, chip, h2):
        red, ru, rd = s[(PREC, m)], s[(RU, m)], s[(RD, m)]
        for h in range(2):
            for d in arrive[h]:
                d.wait_recv()
            q = pl.ds(h * h2, h2)
            total = (red[chip, q] + ru[q] + rd[q]).astype(BF16).astype(F32)
            if kind == 2:
                x = s[srow][q].astype(F32)
                scale = lax.rsqrt(jnp.mean(x * x, axis=-1, keepdims=True) + NORM_EPS)
                s[(GP,)][slot:slot + 1] += jnp.sum(total * x * scale, axis=0, keepdims=True)
                ct = total * s[gain[:1]][gain[1]:gain[1] + 1]
                total = scale * ct - x * (scale * scale * scale) * jnp.mean(ct * x, axis=-1, keepdims=True)
            val = (s[base][q].astype(F32) + total).astype(BF16)
            s[new][q] = val
            if kind == 0:
                val = norm_rows(val.astype(F32), s[gain[:1]][gain[1]:gain[1] + 1]).astype(BF16)
                s[norm][q] = val
            if kind == 1:
                val = s[(GR, m)][q]
            if h == 1:
                for d in drain:
                    d.wait_send()
            if news:
                s[(FN, m)][chip, pl.ds(starts[h], h2)] = val
                for d in news[h][5]:
                    d.start()

    def scores(self, t, keys, q):
        total, rows2 = keys.shape[0], q.shape[0]
        sc = dot_nt(keys, q) * HEAD ** -0.5
        kpos = lax.broadcasted_iota(jnp.int32, (total, rows2), 0)
        qpos = lax.broadcasted_iota(jnp.int32, (total, rows2), 1) + t * rows2
        return jnp.where(kpos <= qpos, sc, -1e30)

    def heads(self, qkv, span):
        ow, total = self.plan.mix_w, 2 * span * self.plan.rows
        return (qkv[:span, :, ow:ow + HEAD].reshape(total, HEAD), qkv[:span, :, ow + HEAD:ow + 2 * HEAD].reshape(total, HEAD))

    def attn_f(self, s, need, loop, hook, m, l, full, early, bare):
        need((WQ, l), (WO, l))
        qkv, mix, lse = s[(QKV, m, l)], s[(MIX, m, l)], s[(LSE, m, l)]

        def proj(t):
            qkv[t] = dot_nn(full[t], s[(WQ, l)][...]).astype(BF16)
        loop(proj)

        def attend(span, t):
            keys, vals = self.heads(qkv, span)
            for h in range(self.plan.mix_w // HEAD):
                cols = slice(h * HEAD, (h + 1) * HEAD)
                sc = self.scores(t, keys, qkv[t, :, cols])
                top = jnp.max(sc, axis=0, keepdims=True)
                ex = jnp.exp(sc - top)
                tot = jnp.sum(ex, axis=0, keepdims=True)
                lse[t, h:h + 1] = top + jnp.log(tot)
                mix[t, :, cols] = dot_tn((ex * (1.0 / tot)).astype(BF16), vals).astype(BF16)
            s[(PART,)][t] = dot_nn(mix[t], s[(WO, l)][...])
        size = 1 if bare else self.plan.chips // 2
        for lo in range(0, self.plan.chips, size):
            loop(functools.partial(attend, lo + size), m, hook if lo <= 1 < lo + size else None, 1, lo, lo + size)

    def mlp_f(self, s, need, loop, hook, m, l, full, early, bare):
        need((W1, l), (W3, l), (W2, l))

        def tile(t):
            v = full[t]
            g = dot_nn(v, s[(W1, l)][...])
            w = dot_nn(v, s[(W3, l)][...])
            s[(PART,)][t] = dot_nn((g * jax.nn.sigmoid(g) * w).astype(BF16), s[(W2, l)][...])
        loop(tile, m)
        if hook is not None:
            hook()

    def start_sums(self, s, need, m, keys):
        for key in keys:
            if m > 0:
                need(key)
            else:
                s[key][...] = jnp.zeros_like(s[key])

    def mlp_b(self, s, need, loop, hook, m, l, full, early, bare):
        need((W1, l), (W3, l), (W2, l))
        self.start_sums(s, need, m, ((A1,), (A3,), (A2,)))
        grad = s[(FN, m)]

        def tile(t):
            v, dy = full[t], grad[t]
            g = dot_nn(v, s[(W1, l)][...])
            w = dot_nn(v, s[(W3, l)][...])
            sig = jax.nn.sigmoid(g)
            act = g * sig
            s[(A2,)][...] += dot_tn((act * w).astype(BF16), dy)
            dm = dot_nt(dy, s[(W2, l)][...]).astype(BF16).astype(F32)
            dw = (dm * act).astype(BF16)
            dg = (dm * w * sig * (1.0 + g * (1.0 - sig))).astype(BF16)
            s[(A1,)][...] += dot_tn(v, dg)
            s[(A3,)][...] += dot_tn(v, dw)
            s[(PART,)][t] = dot_nt(dg, s[(W1, l)][...]) + dot_nt(dw, s[(W3, l)][...])
        loop(tile, m, hook, 2)

    def attn_b(self, s, need, loop, hook, m, l, full, early, bare):
        need((WQ, l), (WO, l), (QKV, m, l), (MIX, m, l), (LSE, m, l))
        self.start_sums(s, need, m, ((AQ,), (AO,)))
        grad, dqkv, dk, dv = s[(FN, m)], s[(DQKV,)], s[(DK,)], s[(DV,)]
        qkv, mix, lse = s[(QKV, m, l)], s[(MIX, m, l)], s[(LSE, m, l)]
        dk[...] = jnp.zeros_like(dk)
        dv[...] = jnp.zeros_like(dv)

        def attend(span, t):
            size = 2 * span * self.plan.rows
            dh = grad[t]
            if not bare:
                s[(AO,)][...] += dot_tn(mix[t], dh)
            do = dot_nt(dh, s[(WO, l)][...]).astype(BF16)
            keys, vals = self.heads(qkv, span)
            for h in range(self.plan.mix_w // HEAD):
                cols = slice(h * HEAD, (h + 1) * HEAD)
                q, doh = qkv[t, :, cols], do[:, cols]
                prob = jnp.exp(self.scores(t, keys, q) - lse[t, h:h + 1])
                dv[:size] += dot_nn(prob.astype(BF16), doh)
                dp = dot_nt(vals, doh).astype(BF16).astype(F32)
                rd = jnp.sum(dp * prob, axis=0, keepdims=True)
                ds = (prob * (dp - rd) * HEAD ** -0.5).astype(BF16)
                dk[:size] += dot_nn(ds, q)
                dqkv[t, :, cols] = dot_tn(ds, keys).astype(BF16)
        step = 1 if bare else self.plan.chips // 2
        for lo in range(0, self.plan.chips, step):
            loop(functools.partial(attend, lo + step), None, hook if lo <= 2 < lo + step else None, 2, lo, lo + step)
        ow, shp = self.plan.mix_w, dqkv.shape[:2] + (HEAD,)
        dqkv[:, :, ow:ow + HEAD] = dk[...].astype(BF16).reshape(shp)
        dqkv[:, :, ow + HEAD:ow + 2 * HEAD] = dv[...].astype(BF16).reshape(shp)

        def tile(t):
            if not bare:
                s[(AQ,)][...] += dot_tn(full[t], dqkv[t])
            s[(PART,)][t] = dot_nt(dqkv[t], s[(WQ, l)][...])
        loop(tile, m, None if l else early, 2, spin=True)

        def sums(t):
            s[(AO,)][...] += dot_tn(mix[t], grad[t])
            s[(AQ,)][...] += dot_tn(full[t], dqkv[t])
        return functools.partial(loop, sums) if bare else None

    def run(self, state):
        any_spec = pl.BlockSpec(memory_space=pl.ANY)
        pn = self.plan
        self.arrays, self.place = [], {}
        for key in self.live_in:
            arr, idx = state[key]
            found = [q for q, other in enumerate(self.arrays) if other is arr]
            if not found:
                self.arrays.append(arr)
            self.place[key] = (found[0] if found else len(self.arrays) - 1, idx)
        self.stacks = []
        for key in self.results:
            if key[:1] not in self.stacks:
                self.stacks.append(key[:1])
        shapes = [self.out_shape(key) for key in self.live_out]
        for kind in self.stacks:
            shp, dtype = pn.shape(kind)
            lead = () if kind == (GSUM,) else (pn.micro,) if kind[0] in (YR, GR) else (pn.layers,)
            shapes.append(jax.ShapeDtypeStruct(lead + shp, dtype))
        vals = pl.pallas_call(
            self.body,
            out_shape=shapes,
            in_specs=[any_spec] * len(self.arrays),
            out_specs=[any_spec] * len(shapes),
            scratch_shapes=[pltpu.VMEM(*pn.shape(key)) for key in self.keys] + [
                pltpu.SemaphoreType.DMA((len(self.live_in) + len(self.live_out) + len(self.results),)),
                pltpu.SemaphoreType.DMA((pn.micro, 52)), pltpu.SemaphoreType.DMA((pn.micro, 52)),
                pltpu.SemaphoreType.DMA((pn.micro, pn.chips)), pltpu.SemaphoreType.DMA((pn.micro, pn.chips))],
            compiler_params=pltpu.CompilerParams(collective_id=self.cid, has_side_effects=True, vmem_limit_bytes=VMEM_BYTES),
        )(*self.arrays)
        state.update(zip(self.live_out + self.stacks, [(v, None) for v in vals]))


def hand_over(arrays):
    n = len(arrays)

    def body(*refs):
        src, dst, tmp, sem = refs[:n], refs[n:2 * n], refs[2 * n:3 * n], refs[3 * n]
        first = [pltpu.make_async_copy(src[q], tmp[q], sem.at[0, q]) for q in range(n)]
        second = [pltpu.make_async_copy(tmp[q], dst[q], sem.at[1, q]) for q in range(n)]
        for d in first:
            d.start()
        for q in range(n):
            first[q].wait()
            second[q].start()
        for d in second:
            d.wait()

    any_spec = pl.BlockSpec(memory_space=pl.ANY)
    return pl.pallas_call(
        body, out_shape=[jax.ShapeDtypeStruct(a.shape, a.dtype) for a in arrays],
        in_specs=[any_spec] * n, out_specs=[any_spec] * n,
        scratch_shapes=[pltpu.VMEM(a.shape, a.dtype) for a in arrays] + [pltpu.SemaphoreType.DMA((2, n))],
        compiler_params=pltpu.CompilerParams(vmem_limit_bytes=VMEM_BYTES))(*arrays)


def solution(mesh):
    rows_p = P(None, ('dp', 'tp'), None)
    flat = P(None, None)
    cols_p = P(None, None, 'tp')
    head_p = P(None, 'tp', None, None)
    down_p = P(None, 'tp', None)
    count = mesh.shape['tp']

    def device_program(x_in, y_cot, gain_attn, gain_mlp, w_qkv, w_out, w_gate, w_up, w_down):
        micro, rows, width = x_in.shape
        layers = w_qkv.shape[0]
        wq = w_qkv.reshape(layers, width, -1)
        wo = w_out.reshape(layers, -1, width)
        plan = Plan(count, micro, layers, rows, width, wq.shape[2], wo.shape[1], w_gate.shape[2])
        state = {(GA,): (gain_attn, None), (GM,): (gain_mlp, None)}
        for m in range(micro):
            state[(XR, m, 0)], state[(GR, m)] = (x_in, m), (y_cot, m)
        for l in range(layers):
            for key, arr in ((WQ, wq), (WO, wo), (W1, w_gate), (W3, w_up), (W2, w_down)):
                state[(key, l)] = (arr, l)
        cuts = [0] + list(SPLITS) + [len(plan.seq)]
        for cid in range(len(cuts) - 1):
            Kernel(plan, cid, cuts[cid], cuts[cid + 1]).run(state)
        y_out, grad_x, g_out, g_gate, g_up, g_down, gsum = hand_over([state[(x,)][0] for x in (YR, GR, BO, B1, B3, B2, GSUM)])
        return (y_out, grad_x, state[(BQ,)][0].reshape(w_qkv.shape), g_out.reshape(w_out.shape), g_gate, g_up, g_down,
                gsum[:layers], gsum[layers:])

    return jax.shard_map(device_program, mesh=mesh,
                         in_specs=(rows_p, rows_p, flat, flat, P(None, None, 'tp', None, None), head_p, cols_p, cols_p, down_p),
                         out_specs=(rows_p, rows_p, P('dp', None, 'tp', None, None), P('dp', 'tp', None, None), P('dp', None, 'tp'),
                                    P('dp', None, 'tp'), P('dp', 'tp', None), P('dp', None), P('dp', None)),
                         check_vma=False)
```
